32 devices in a mesh: replica: 4 (over y, core), shard: 8 (over z, x).
Axes of the slice: x: 2, y: 2, z: 4, core: 2. Of those that a mesh axis runs over, the one named last changes fastest.
Arguments:
- anchor: float32 [384, 8192], P('shard'), may hold values from -6 to 6
- replica_rows: bfloat16 [4, 384, 8192], P('replica', 'shard'), may hold values from -6 to 6
- outer_velocity: float32 [384, 8192], P('shard', 'replica'), may hold values from -6 to 6
- features: bfloat16 [4, 384, 256], P('replica', 'shard'), may hold values from -6 to 6
- cotangent: bfloat16 [4, 256, 1024], P('replica', 'shard'), may hold values from -0.375 to 0.375
- inner_weight: float32 [4, 384, 1024], P('replica', 'shard'), may hold values from -6 to 6
- first_moment: float32 [4, 384, 1024], P('replica', 'shard'), may hold values from -6 to 6
- second_moment: float32 [4, 384, 1024], P('replica', 'shard'), may hold values from 0.5 to 2
Outputs:
- new_anchor: float32 [384, 8192], P('shard')
- merged_rows: bfloat16 [4, 384, 8192], P('replica', 'shard')
- new_velocity: float32 [384, 8192], P('shard', 'replica')
- new_weight: float32 [4, 384, 1024], P('replica', 'shard')
- new_first: float32 [4, 384, 1024], P('replica', 'shard')
- new_second: float32 [4, 384, 1024], P('replica', 'shard')
The draws below stay inside these ranges and needn't reach their ends.
All inputs are finite; a program needn't handle non-finite values.
Results may differ from the reference program's by a relative error of at most 0.0035.
Values may be sent and summed in bfloat16 or wider, within the bound.
A program may use at most 64 MiB of HBM per device.

```python
import math
import jax
import jax.numpy as jnp
from jax import lax

D = 8192
KV = 1024
DW = 384
TOK = 256
N_REPLICA = 4


def shard_levels(stream_key, dims, split, smallest, high):
    def one(axis_at, parts):
        heights = jax.random.uniform(jax.random.fold_in(jax.random.fold_in(stream_key, 6), axis_at), (parts,), jnp.float32, smallest / len(split), high / len(split))
        return jnp.repeat(jnp.exp(heights), dims[axis_at] // parts).reshape((-1,) + (1,) * (len(dims) - axis_at - 1))

    level = one(*split[0])
    for cut in split[1:]:
        level = level * one(*cut)
    return level


def centred(key, extent, width, reach, shards=(), kind=jnp.bfloat16):
    factor_of = shard_levels(key, extent, shards, -0.22, 0.18) if shards else 1.0
    array = jax.random.normal(key, extent, jnp.float32) * width * factor_of
    return jnp.minimum(jnp.maximum(array, -reach), reach).astype(kind)


def setup_inputs(seed: int = 0) -> dict:
    splits = jax.random.split(jax.random.key(seed), 9)
    return {
        "anchor": centred(splits[0], (DW, D), 1.0, 6.0, ((0, 8),), jnp.float32),
        "replica_rows": centred(splits[1], (N_REPLICA, DW, D), 1.0, 6.0, ((0, 4), (1, 8))),
        "outer_velocity": centred(splits[2], (DW, D), 0.5, 6.0, ((0, 8), (1, 4)), jnp.float32),
        "features": centred(splits[3], (N_REPLICA, DW, TOK), 1.0, 6.0, ((0, 4), (1, 8))),
        "cotangent": centred(splits[4], (N_REPLICA, TOK, KV), TOK ** -0.5, 0.375, ((0, 4), (1, 8))),
        "inner_weight": centred(splits[5], (N_REPLICA, DW, KV), 1.0, 6.0, ((0, 4), (1, 8)), jnp.float32),
        "first_moment": centred(splits[6], (N_REPLICA, DW, KV), 0.5, 6.0, ((0, 4), (1, 8)), jnp.float32),
        "second_moment": jnp.clip(jnp.exp(math.log(2.0) - 1.3862944 * jax.random.uniform(splits[7], (N_REPLICA, DW, KV), jnp.float32) ** shard_levels(splits[7], (N_REPLICA, DW, KV), ((0, 4), (1, 8)), -0.2, 0.2)), 0.5, 2.0),
    }


momentum_keep = 0.9
outer_rate = 0.7
blend_keep = 0.5
inner_rate = 0.01
decay_first = 0.9
decay_second = 0.95
weight_decay = 0.1
epsilon = 1e-08
first_fix = 1.0 - 0.9 ** 10
second_fix = 1.0 - 0.95 ** 10

def reference(anchor, replica_rows, outer_velocity, features, cotangent, inner_weight, first_moment, second_moment):
    drift = anchor[None] - replica_rows.astype(jnp.float32)
    outer_grad = lax.optimization_barrier(jnp.sum(drift, axis=0)) / N_REPLICA
    new_velocity = momentum_keep * outer_velocity + outer_grad
    new_anchor = anchor - outer_rate * (outer_grad + momentum_keep * new_velocity)
    merged_rows = (blend_keep * replica_rows.astype(jnp.float32) + (1.0 - blend_keep) * new_anchor[None]).astype(jnp.bfloat16)
    gradient = jnp.einsum('rdt,rtk->rdk', features.astype(jnp.float32), cotangent.astype(jnp.float32), precision=lax.Precision.HIGHEST)
    new_first = decay_first * first_moment + (1.0 - decay_first) * gradient
    new_second = decay_second * second_moment + (1.0 - decay_second) * gradient * gradient
    stepped = new_first / first_fix / (jnp.sqrt(new_second / second_fix) + epsilon)
    new_weight = inner_weight - inner_rate * (stepped + weight_decay * inner_weight)
    return (new_anchor, merged_rows, new_velocity, new_weight, new_first, new_second)
```

```python
import functools

import jax
import jax.numpy as jnp
from jax import lax
from jax.experimental import pallas as pl
from jax.experimental.pallas import tpu as pltpu
from jax.sharding import PartitionSpec as P

momentum_keep = 0.9
outer_rate = 0.7
blend_keep = 0.5
inner_rate = 0.01
decay_first = 0.9
decay_second = 0.95
weight_decay = 0.1
epsilon = 1e-08
first_fix = 1.0 - 0.9**10
second_fix = 1.0 - 0.95**10

MESH = pl.DeviceIdType.MESH
SPLIT = 4


def kernel(R, S, anchor_h, rows_h, vel_h, feat_h, cot_h, w_h, m_h, s_h,
           na_o, mg_o, nv_o, nw_o, nm_o, ns_o,
           anchor, rows, vel, feat, cot, w, m, s, sib_rows, msg,
           in_sem, sib_send, sib_recv, y_send, fwd_send, msg_recv,
           cot_own_send, cot_z_send, cot_x_send, cot_recv):
    C = R // 2
    H = SPLIT
    me, at = lax.axis_index("replica"), lax.axis_index("shard")
    y, c = me // 2, me % 2
    sib = me + 1 - 2 * c
    partner = at + 1 - 2 * (at % 2)
    pos, length = at // 2, S // 2
    W = vel.shape[1]
    piece = W // H
    depth = cot_h.shape[1]

    def columns(q, h):
        return pl.ds(pl.multiple_of(q * W + h * piece, 128), piece)

    def quarter(q):
        return pl.ds(pl.multiple_of(q * W, 128), W)

    def tokens(k):
        return pl.ds(pl.multiple_of(k * depth, depth), depth)

    barrier = pltpu.get_barrier_semaphore()
    pl.semaphore_signal(barrier, inc=1, device_id={"replica": sib}, device_id_type=MESH)
    for t in range(1, C):
        pl.semaphore_signal(barrier, inc=1, device_id={"replica": lax.rem(me + 2 * t, R)}, device_id_type=MESH)
    pl.semaphore_signal(barrier, inc=1, device_id={"shard": partner}, device_id_type=MESH)

    @pl.when(pos > 0)
    def _():
        pl.semaphore_signal(barrier, inc=1, device_id={"shard": at - 2}, device_id_type=MESH)

    @pl.when(pos < length - 1)
    def _():
        pl.semaphore_signal(barrier, inc=1, device_id={"shard": at + 2}, device_id_type=MESH)

    loads = {}
    slot = 0

    def load(name, src, dst):
        nonlocal slot
        copy = pltpu.make_async_copy(src, dst, in_sem.at[slot])
        copy.start()
        slot += 1
        loads[name] = copy

    load("cot", cot_h.at[0], cot.at[tokens(at)])
    for j in range(C):
        q = 2 * j + 1 - c
        load(("out", j), rows_h.at[0, :, quarter(q)], rows.at[:, quarter(q)])
    for j in range(C):
        q = 2 * j + c
        load(("keep", j), rows_h.at[0, :, quarter(q)], rows.at[:, quarter(q)])
    load("anchor", anchor_h, anchor)
    load("vel", vel_h, vel)
    load("feat", feat_h.at[0], feat)
    load("w", w_h.at[0], w)
    load("m", m_h.at[0], m)
    load("s", s_h.at[0], s)

    count = 2 + (C - 1) + (pos > 0).astype(jnp.int32) + (pos < length - 1).astype(jnp.int32)
    pl.semaphore_wait(barrier, count)

    def sib_copy(j, h):
        return pltpu.make_async_remote_copy(
            src_ref=rows.at[:, columns(2 * j + 1 - c, h)], dst_ref=sib_rows.at[j, h],
            send_sem=sib_send.at[j, h], recv_sem=sib_recv.at[j, h],
            device_id={"replica": sib}, device_id_type=MESH)

    def cot_copy(k, send_sem, target):
        return pltpu.make_async_remote_copy(
            src_ref=cot.at[tokens(k)], dst_ref=cot.at[tokens(k)],
            send_sem=send_sem, recv_sem=cot_recv.at[k],
            device_id={"shard": target}, device_id_type=MESH)

    for j in range(C):
        loads[("out", j)].wait()
        for h in range(H):
            sib_copy(j, h).start()

    loads["cot"].wait()
    cot_right = cot_copy(at, cot_own_send.at[0], at + 2)
    cot_left = cot_copy(at, cot_own_send.at[1], at - 2)
    cot_across = cot_copy(at, cot_own_send.at[2], partner)

    @pl.when(pos < length - 1)
    def _():
        cot_right.start()

    @pl.when(pos > 0)
    def _():
        cot_left.start()

    cot_across.start()

    def y_copy(t, j, h):
        return pltpu.make_async_remote_copy(
            src_ref=msg.at[c, y, j, h], dst_ref=msg.at[c, y, j, h],
            send_sem=y_send.at[t - 1, j, h], recv_sem=msg_recv.at[c, y, j, h],
            device_id={"replica": lax.rem(me + 2 * t, R)}, device_id_type=MESH)

    def to_sib(src, j, h):
        return pltpu.make_async_remote_copy(
            src_ref=msg.at[c, src, j, h], dst_ref=msg.at[c, src, j, h],
            send_sem=fwd_send.at[src, j, h], recv_sem=msg_recv.at[c, src, j, h],
            device_id={"replica": sib}, device_id_type=MESH)

    def arrival(p, src, j, h):
        return pltpu.make_async_remote_copy(
            src_ref=msg.at[p, src, j, h], dst_ref=msg.at[p, src, j, h],
            send_sem=fwd_send.at[src, j, h], recv_sem=msg_recv.at[p, src, j, h],
            device_id={"replica": sib}, device_id_type=MESH)

    c1 = outer_rate * (1.0 + momentum_keep)
    c2 = outer_rate * momentum_keep * momentum_keep
    share = c1 / R
    for j in range(C):
        loads[("keep", j)].wait()
        if j == 0:
            loads["anchor"].wait()
            loads["vel"].wait()
        mine = y == j
        of_anchor = jnp.where(mine, 0.0, 2.0)
        of_rows = jnp.where(mine, share, -1.0)
        of_vel = jnp.where(mine, -c2, 0.0)
        for h in range(H):
            sib_copy(j, h).wait_recv()
            cols = columns(2 * j + c, h)
            both = rows[:, cols].astype(jnp.float32) + sib_rows[j, h].astype(jnp.float32)
            value = of_anchor * anchor[:, cols] + of_rows * both
            value = value + of_vel * vel[:, h * piece:(h + 1) * piece]
            msg[c, y, j, h] = value.astype(jnp.bfloat16)
            for t in range(1, C):
                y_copy(t, j, h).start()
            to_sib(y, j, h).start()

    def finish(p, j, h):
        cols = columns(2 * j + p, h)
        others = msg[p, (j + 1) % C, j, h].astype(jnp.float32)
        for t in range(2, C):
            others = others + msg[p, (j + t) % C, j, h].astype(jnp.float32)
        own = msg[p, j, j, h].astype(jnp.float32)
        new_anchor = (1.0 - 2.0 * share) * anchor[:, cols] + own - share * others
        na_o[:, cols] = new_anchor
        mg_o[0, :, cols] = (
            blend_keep * rows[:, cols].astype(jnp.float32) + (1.0 - blend_keep) * new_anchor
        ).astype(jnp.bfloat16)

    def finish_velocity(j, h):
        @pl.when(y == j)
        def _():
            cols = columns(2 * j + c, h)
            part = slice(h * piece, (h + 1) * piece)
            total = 2.0 * anchor[:, cols] - (
                rows[:, cols].astype(jnp.float32) + sib_rows[j, h].astype(jnp.float32))
            for t in range(1, C):
                total = total + msg[c, (j + t) % C, j, h].astype(jnp.float32)
            nv_o[:, part] = momentum_keep * vel[:, part] + total / R

    def finish_sib(j, h):
        for src in range(C):
            arrival(1 - c, src, j, h).wait_recv()
        finish(1 - c, j, h)

    def cot_step(t):
        @pl.when(pos >= t)
        def _():
            k = at - 2 * t
            cot_copy(k, cot_x_send.at[0], partner).wait_recv()

            @pl.when(pos < length - 1)
            def _():
                cot_copy(k, cot_z_send.at[0, t - 1], at + 2).start()

            cot_copy(k, cot_x_send.at[k // 2], partner).start()

        @pl.when(pos + t < length)
        def _():
            k = at + 2 * t
            cot_copy(k, cot_x_send.at[0], partner).wait_recv()

            @pl.when(pos > 0)
            def _():
                cot_copy(k, cot_z_send.at[1, t - 1], at - 2).start()

            cot_copy(k, cot_x_send.at[k // 2], partner).start()

    steps = length - 1
    pieces = [(j, h) for j in range(C) for h in range(H)]
    done = 0
    before = None
    for i, (j, h) in enumerate(pieces):
        for t in range(1, C):
            src = lax.rem(y + t, C)
            arrival(c, src, j, h).wait_recv()
            to_sib(src, j, h).start()
        finish(c, j, h)
        finish_velocity(j, h)
        if before is not None:
            finish_sib(*before)
        before = (j, h)
        goal = min(steps, (i + 1) * steps // (len(pieces) - 1))
        while done < goal:
            done += 1
            cot_step(done)

    for k in range(length):
        cot_copy(2 * k + 1 - at % 2, cot_x_send.at[0], partner).wait_recv()
    for name in ("feat", "w", "m", "s"):
        loads[name].wait()
    tile = min(256, w.shape[1])
    for n in range(w.shape[1] // tile):
        part = slice(n * tile, (n + 1) * tile)
        gradient = jnp.dot(feat[...], cot[:, part], preferred_element_type=jnp.float32)
        new_first = decay_first * m[:, part] + (1.0 - decay_first) * gradient
        new_second = decay_second * s[:, part] + (1.0 - decay_second) * gradient * gradient
        stepped = new_first / first_fix / (jnp.sqrt(new_second / second_fix) + epsilon)
        weight = w[:, part]
        nw_o[0, :, part] = weight - inner_rate * (stepped + weight_decay * weight)
        nm_o[0, :, part] = new_first
        ns_o[0, :, part] = new_second

    finish_sib(*before)

    for j, h in pieces:
        sib_copy(j, h).wait_send()
        for t in range(1, C):
            y_copy(t, j, h).wait_send()
        for src in range(C):
            to_sib(src, j, h).wait_send()
    cot_across.wait_send()

    @pl.when(pos < length - 1)
    def _():
        cot_right.wait_send()

    @pl.when(pos > 0)
    def _():
        cot_left.wait_send()

    for t in range(1, length):
        @pl.when(pos >= t)
        def _():
            @pl.when(pos < length - 1)
            def _():
                cot_copy(at - 2 * t, cot_z_send.at[0, t - 1], at + 2).wait_send()

            cot_copy(at - 2 * t, cot_x_send.at[(at - 2 * t) // 2], partner).wait_send()

        @pl.when(pos + t < length)
        def _():
            @pl.when(pos > 0)
            def _():
                cot_copy(at + 2 * t, cot_z_send.at[1, t - 1], at - 2).wait_send()

            cot_copy(at + 2 * t, cot_x_send.at[(at + 2 * t) // 2], partner).wait_send()


def local(R, S, anchor, replica_rows, outer_velocity, features, cotangent,
          inner_weight, first_moment, second_moment):
    C, H = R // 2, SPLIT
    depth_rows = anchor.shape[0]
    W = outer_velocity.shape[1]
    f32, bf16 = jnp.float32, jnp.bfloat16
    args = (anchor, replica_rows, outer_velocity, features, cotangent,
            inner_weight, first_moment, second_moment)
    outs = (anchor, replica_rows, outer_velocity, inner_weight, first_moment, second_moment)
    dma = pltpu.SemaphoreType.DMA
    length = S // 2
    room = 67043328 - sum(a.size * a.dtype.itemsize for a in outs) - 2**16
    return pl.pallas_call(
        functools.partial(kernel, R, S),
        out_shape=tuple(pltpu.VMEM(a.shape, a.dtype) for a in outs),
        in_specs=[pl.BlockSpec(memory_space=pltpu.HBM)] * len(args),
        out_specs=tuple(pl.BlockSpec(memory_space=pltpu.VMEM) for _ in outs),
        scratch_shapes=[
            pltpu.VMEM(anchor.shape, f32),
            pltpu.VMEM(replica_rows.shape[1:], bf16),
            pltpu.VMEM(outer_velocity.shape, f32),
            pltpu.VMEM(features.shape[1:], bf16),
            pltpu.VMEM((S * cotangent.shape[1], cotangent.shape[2]), bf16),
            pltpu.VMEM(inner_weight.shape[1:], f32),
            pltpu.VMEM(inner_weight.shape[1:], f32),
            pltpu.VMEM(inner_weight.shape[1:], f32),
            pltpu.VMEM((C, H, depth_rows, W // H), bf16),
            pltpu.VMEM((2, C, C, H, depth_rows, W // H), bf16),
            dma((7 + 2 * C,)),
            dma((C, H)),
            dma((C, H)),
            dma((C - 1, C, H)),
            dma((C, C, H)),
            dma((2, C, C, H)),
            dma((3,)),
            dma((2, max(length - 1, 1))),
            dma((length,)),
            dma((S,)),
        ],
        compiler_params=pltpu.CompilerParams(
            collective_id=0, has_side_effects=True, vmem_limit_bytes=room),
    )(*args)


def solution(mesh):
    in_specs = (
        P("shard", None),
        P("replica", "shard", None),
        P("shard", "replica"),
        P("replica", "shard", None),
        P("replica", "shard", None),
        P("replica", "shard", None),
        P("replica", "shard", None),
        P("replica", "shard", None),
    )
    out_specs = (
        P("shard", None),
        P("replica", "shard", None),
        P("shard", "replica"),
        P("replica", "shard", None),
        P("replica", "shard", None),
        P("replica", "shard", None),
    )
    body = functools.partial(local, mesh.shape["replica"], mesh.shape["shard"])
    return jax.shard_map(body, mesh=mesh, in_specs=in_specs, out_specs=out_specs, check_vma=False)
```

```python
import functools

import jax
import jax.numpy as jnp
from jax import lax
from jax.experimental import pallas as pl
from jax.experimental.pallas import tpu as pltpu
from jax.sharding import PartitionSpec as P

momentum_keep = 0.9
outer_rate = 0.7
blend_keep = 0.5
inner_rate = 0.01
decay_first = 0.9
decay_second = 0.95
weight_decay = 0.1
epsilon = 1e-08
first_fix = 1.0 - 0.9**10
second_fix = 1.0 - 0.95**10

MESH = pl.DeviceIdType.MESH
SPLIT = 4
PARTS = 2


def kernel(R, S, anchor_h, rows_h, vel_h, feat_h, cot_h, w_h, m_h, s_h,
           na_o, mg_o, nv_o, nw_o, nm_o, ns_o,
           anchor, rows, vel, feat, cot, w, m, s, sib_rows, msg,
           in_sem, sib_send, sib_recv, y_send, fwd_send, msg_recv,
           cot_own_send, cot_z_send, cot_x_send, cot_recv):
    C = R // 2
    H = SPLIT
    me, at = lax.axis_index("replica"), lax.axis_index("shard")
    y, c = me // 2, me % 2
    sib = me + 1 - 2 * c
    partner = at + 1 - 2 * (at % 2)
    pos, length = at // 2, S // 2
    W = vel.shape[1]
    piece = W // H
    depth = cot_h.shape[1]
    part_depth = depth // PARTS

    def columns(q, h):
        return pl.ds(pl.multiple_of(q * W + h * piece, 128), piece)

    def quarter(q):
        return pl.ds(pl.multiple_of(q * W, 128), W)

    def tokens(k):
        return pl.ds(pl.multiple_of(k * depth, depth), depth)

    def half_tokens(k, u):
        return pl.ds(pl.multiple_of(k * depth + u * part_depth, part_depth), part_depth)

    barrier = pltpu.get_barrier_semaphore()
    pl.semaphore_signal(barrier, inc=1, device_id={"replica": sib}, device_id_type=MESH)
    for t in range(1, C):
        pl.semaphore_signal(barrier, inc=1, device_id={"replica": lax.rem(me + 2 * t, R)}, device_id_type=MESH)
    pl.semaphore_signal(barrier, inc=1, device_id={"shard": partner}, device_id_type=MESH)

    @pl.when(pos > 0)
    def _():
        pl.semaphore_signal(barrier, inc=1, device_id={"shard": at - 2}, device_id_type=MESH)

    @pl.when(pos < length - 1)
    def _():
        pl.semaphore_signal(barrier, inc=1, device_id={"shard": at + 2}, device_id_type=MESH)

    loads = {}
    slot = 0

    def load(name, src, dst):
        nonlocal slot
        copy = pltpu.make_async_copy(src, dst, in_sem.at[slot])
        copy.start()
        slot += 1
        loads[name] = copy

    load("cot", cot_h.at[0], cot.at[tokens(at)])
    for j in range(C):
        q = 2 * j + 1 - c
        load(("out", j), rows_h.at[0, :, quarter(q)], rows.at[:, quarter(q)])
    for j in range(C):
        q = 2 * j + c
        load(("keep", j), rows_h.at[0, :, quarter(q)], rows.at[:, quarter(q)])
    load("anchor", anchor_h, anchor)
    load("vel", vel_h, vel)
    load("feat", feat_h.at[0], feat)
    load("w", w_h.at[0], w)
    load("m", m_h.at[0], m)
    load("s", s_h.at[0], s)

    count = 2 + (C - 1) + (pos > 0).astype(jnp.int32) + (pos < length - 1).astype(jnp.int32)
    pl.semaphore_wait(barrier, count)

    def sib_copy(j, h):
        return pltpu.make_async_remote_copy(
            src_ref=rows.at[:, columns(2 * j + 1 - c, h)], dst_ref=sib_rows.at[j, h],
            send_sem=sib_send.at[j, h], recv_sem=sib_recv.at[j, h],
            device_id={"replica": sib}, device_id_type=MESH)

    def cot_copy(k, u, send_sem, target):
        return pltpu.make_async_remote_copy(
            src_ref=cot.at[half_tokens(k, u)], dst_ref=cot.at[half_tokens(k, u)],
            send_sem=send_sem.at[u], recv_sem=cot_recv.at[k, u],
            device_id={"shard": target}, device_id_type=MESH)

    for j in range(C):
        loads[("out", j)].wait()
        for h in range(H):
            sib_copy(j, h).start()

    loads["cot"].wait()
    cot_right = [cot_copy(at, u, cot_own_send.at[0], at + 2) for u in range(PARTS)]
    cot_left = [cot_copy(at, u, cot_own_send.at[1], at - 2) for u in range(PARTS)]
    cot_across = [cot_copy(at, u, cot_own_send.at[2], partner) for u in range(PARTS)]

    @pl.when(pos < length - 1)
    def _():
        for copy in cot_right:
            copy.start()

    @pl.when(pos > 0)
    def _():
        for copy in cot_left:
            copy.start()

    for copy in cot_across:
        copy.start()

    def y_copy(t, j, h):
        return pltpu.make_async_remote_copy(
            src_ref=msg.at[c, y, j, h], dst_ref=msg.at[c, y, j, h],
            send_sem=y_send.at[t - 1, j, h], recv_sem=msg_recv.at[c, y, j, h],
            device_id={"replica": lax.rem(me + 2 * t, R)}, device_id_type=MESH)

    def to_sib(src, j, h):
        return pltpu.make_async_remote_copy(
            src_ref=msg.at[c, src, j, h], dst_ref=msg.at[c, src, j, h],
            send_sem=fwd_send.at[src, j, h], recv_sem=msg_recv.at[c, src, j, h],
            device_id={"replica": sib}, device_id_type=MESH)

    def arrival(p, src, j, h):
        return pltpu.make_async_remote_copy(
            src_ref=msg.at[p, src, j, h], dst_ref=msg.at[p, src, j, h],
            send_sem=fwd_send.at[src, j, h], recv_sem=msg_recv.at[p, src, j, h],
            device_id={"replica": sib}, device_id_type=MESH)

    c1 = outer_rate * (1.0 + momentum_keep)
    c2 = outer_rate * momentum_keep * momentum_keep
    share = c1 / R
    for j in range(C):
        loads[("keep", j)].wait()
        if j == 0:
            loads["anchor"].wait()
            loads["vel"].wait()
        mine = y == j
        of_anchor = jnp.where(mine, 0.0, 2.0)
        of_rows = jnp.where(mine, share, -1.0)
        of_vel = jnp.where(mine, -c2, 0.0)
        for h in range(H):
            sib_copy(j, h).wait_recv()
            cols = columns(2 * j + c, h)
            both = rows[:, cols].astype(jnp.float32) + sib_rows[j, h].astype(jnp.float32)
            value = of_anchor * anchor[:, cols] + of_rows * both
            value = value + of_vel * vel[:, h * piece:(h + 1) * piece]
            msg[c, y, j, h] = value.astype(jnp.bfloat16)
            for t in range(1, C):
                y_copy(t, j, h).start()
            to_sib(y, j, h).start()

    def finish(p, j, h):
        cols = columns(2 * j + p, h)
        others = msg[p, (j + 1) % C, j, h].astype(jnp.float32)
        for t in range(2, C):
            others = others + msg[p, (j + t) % C, j, h].astype(jnp.float32)
        own = msg[p, j, j, h].astype(jnp.float32)
        new_anchor = (1.0 - 2.0 * share) * anchor[:, cols] + own - share * others
        na_o[:, cols] = new_anchor
        mg_o[0, :, cols] = (
            blend_keep * rows[:, cols].astype(jnp.float32) + (1.0 - blend_keep) * new_anchor
        ).astype(jnp.bfloat16)

    def finish_velocity(j, h):
        @pl.when(y == j)
        def _():
            cols = columns(2 * j + c, h)
            part = slice(h * piece, (h + 1) * piece)
            total = 2.0 * anchor[:, cols] - (
                rows[:, cols].astype(jnp.float32) + sib_rows[j, h].astype(jnp.float32))
            for t in range(1, C):
                total = total + msg[c, (j + t) % C, j, h].astype(jnp.float32)
            nv_o[:, part] = momentum_keep * vel[:, part] + total / R

    def finish_sib(j, h):
        for src in range(C):
            arrival(1 - c, src, j, h).wait_recv()
        finish(1 - c, j, h)

    def cot_step(t, u):
        @pl.when(pos >= t)
        def _():
            k = at - 2 * t
            cot_copy(k, u, cot_x_send.at[0], partner).wait_recv()

            @pl.when(pos < length - 1)
            def _():
                cot_copy(k, u, cot_z_send.at[0, t - 1], at + 2).start()

            cot_copy(k, u, cot_x_send.at[k // 2], partner).start()

        @pl.when(pos + t < length)
        def _():
            k = at + 2 * t
            cot_copy(k, u, cot_x_send.at[0], partner).wait_recv()

            @pl.when(pos > 0)
            def _():
                cot_copy(k, u, cot_z_send.at[1, t - 1], at - 2).start()

            cot_copy(k, u, cot_x_send.at[k // 2], partner).start()

    pieces = [(j, h) for j in range(C) for h in range(H)]
    todo = [(t, u) for t in range(1, length) for u in range(PARTS)]
    before = None
    for i, (j, h) in enumerate(pieces):
        while todo and 3 * (todo[0][0] - 1) + todo[0][1] <= i + 2:
            cot_step(*todo.pop(0))
        for t in range(1, C):
            src = lax.rem(y + t, C)
            arrival(c, src, j, h).wait_recv()
            to_sib(src, j, h).start()
        finish(c, j, h)
        finish_velocity(j, h)
        if before is not None:
            finish_sib(*before)
        before = (j, h)
    for step in todo:
        cot_step(*step)

    for k in range(length):
        for u in range(PARTS):
            cot_copy(2 * k + 1 - at % 2, u, cot_x_send.at[0], partner).wait_recv()
    for name in ("feat", "w", "m", "s"):
        loads[name].wait()
    tile = min(256, w.shape[1])
    for n in range(w.shape[1] // tile):
        part = slice(n * tile, (n + 1) * tile)
        gradient = jnp.dot(feat[...], cot[:, part], preferred_element_type=jnp.float32)
        new_first = decay_first * m[:, part] + (1.0 - decay_first) * gradient
        new_second = decay_second * s[:, part] + (1.0 - decay_second) * gradient * gradient
        stepped = new_first / first_fix / (jnp.sqrt(new_second / second_fix) + epsilon)
        weight = w[:, part]
        nw_o[0, :, part] = weight - inner_rate * (stepped + weight_decay * weight)
        nm_o[0, :, part] = new_first
        ns_o[0, :, part] = new_second

    finish_sib(*before)

    for j, h in pieces:
        sib_copy(j, h).wait_send()
        for t in range(1, C):
            y_copy(t, j, h).wait_send()
        for src in range(C):
            to_sib(src, j, h).wait_send()
    for copy in cot_across:
        copy.wait_send()

    @pl.when(pos < length - 1)
    def _():
        for copy in cot_right:
            copy.wait_send()

    @pl.when(pos > 0)
    def _():
        for copy in cot_left:
            copy.wait_send()

    for t, u in [(t, u) for t in range(1, length) for u in range(PARTS)]:
        @pl.when(pos >= t)
        def _():
            k = at - 2 * t

            @pl.when(pos < length - 1)
            def _():
                cot_copy(k, u, cot_z_send.at[0, t - 1], at + 2).wait_send()

            cot_copy(k, u, cot_x_send.at[k // 2], partner).wait_send()

        @pl.when(pos + t < length)
        def _():
            k = at + 2 * t

            @pl.when(pos > 0)
            def _():
                cot_copy(k, u, cot_z_send.at[1, t - 1], at - 2).wait_send()

            cot_copy(k, u, cot_x_send.at[k // 2], partner).wait_send()


def store_kernel(*refs):
    sems = refs[-1]
    count = (len(refs) - 1) // 2
    copies = []
    for source, target in zip(refs[:count], refs[count:-1]):
        rows = source.shape[-2]
        cuts = 3 if rows % 48 == 0 else 1
        for n in range(cuts):
            part = pl.ds(n * (rows // cuts), rows // cuts)
            index = (0, part) if len(source.shape) == 3 else (part,)
            copies.append(pltpu.make_async_copy(
                source.at[index], target.at[index], sems.at[len(copies)]))
    for copy in copies:
        copy.start()
    for copy in copies:
        copy.wait()


def store(*arrays):
    return pl.pallas_call(
        store_kernel,
        out_shape=tuple(jax.ShapeDtypeStruct(a.shape, a.dtype) for a in arrays),
        in_specs=[pl.BlockSpec(memory_space=pltpu.VMEM)] * len(arrays),
        out_specs=tuple(pl.BlockSpec(memory_space=pltpu.HBM) for _ in arrays),
        scratch_shapes=[pltpu.SemaphoreType.DMA((3 * len(arrays),))],
        compiler_params=pltpu.CompilerParams(vmem_limit_bytes=2**20),
    )(*arrays)


def local(R, S, anchor, replica_rows, outer_velocity, features, cotangent,
          inner_weight, first_moment, second_moment):
    C, H = R // 2, SPLIT
    depth_rows = anchor.shape[0]
    W = outer_velocity.shape[1]
    f32, bf16 = jnp.float32, jnp.bfloat16
    args = (anchor, replica_rows, outer_velocity, features, cotangent,
            inner_weight, first_moment, second_moment)
    outs = (anchor, replica_rows, outer_velocity, inner_weight, first_moment, second_moment)
    dma = pltpu.SemaphoreType.DMA
    length = S // 2
    room = 67043328 - sum(a.size * a.dtype.itemsize for a in outs) - 2**16
    results = pl.pallas_call(
        functools.partial(kernel, R, S),
        out_shape=tuple(pltpu.VMEM(a.shape, a.dtype) for a in outs),
        in_specs=[pl.BlockSpec(memory_space=pltpu.HBM)] * len(args),
        out_specs=tuple(pl.BlockSpec(memory_space=pltpu.VMEM) for _ in outs),
        scratch_shapes=[
            pltpu.VMEM(anchor.shape, f32),
            pltpu.VMEM(replica_rows.shape[1:], bf16),
            pltpu.VMEM(outer_velocity.shape, f32),
            pltpu.VMEM(features.shape[1:], bf16),
            pltpu.VMEM((S * cotangent.shape[1], cotangent.shape[2]), bf16),
            pltpu.VMEM(inner_weight.shape[1:], f32),
            pltpu.VMEM(inner_weight.shape[1:], f32),
            pltpu.VMEM(inner_weight.shape[1:], f32),
            pltpu.VMEM((C, H, depth_rows, W // H), bf16),
            pltpu.VMEM((2, C, C, H, depth_rows, W // H), bf16),
            dma((7 + 2 * C,)),
            dma((C, H)),
            dma((C, H)),
            dma((C - 1, C, H)),
            dma((C, C, H)),
            dma((2, C, C, H)),
            dma((3, PARTS)),
            dma((2, max(length - 1, 1), PARTS)),
            dma((length, PARTS)),
            dma((S, PARTS)),
        ],
        compiler_params=pltpu.CompilerParams(
            collective_id=0, has_side_effects=True, vmem_limit_bytes=room),
    )(*args)
    return store(*results)


def solution(mesh):
    in_specs = (
        P("shard", None),
        P("replica", "shard", None),
        P("shard", "replica"),
        P("replica", "shard", None),
        P("replica", "shard", None),
        P("replica", "shard", None),
        P("replica", "shard", None),
        P("replica", "shard", None),
    )
    out_specs = (
        P("shard", None),
        P("replica", "shard", None),
        P("shard", "replica"),
        P("replica", "shard", None),
        P("replica", "shard", None),
        P("replica", "shard", None),
    )
    body = functools.partial(local, mesh.shape["replica"], mesh.shape["shard"])
    return jax.shard_map(body, mesh=mesh, in_specs=in_specs, out_specs=out_specs, check_vma=False)
```

```python
import functools

import jax
import jax.numpy as jnp
from jax import lax
from jax.experimental import pallas as pl
from jax.experimental.pallas import tpu as pltpu
from jax.sharding import PartitionSpec as P

momentum_keep = 0.9
outer_rate = 0.7
blend_keep = 0.5
inner_rate = 0.01
decay_first = 0.9
decay_second = 0.95
weight_decay = 0.1
epsilon = 1e-08
first_fix = 1.0 - 0.9**10
second_fix = 1.0 - 0.95**10

MESH = pl.DeviceIdType.MESH
SPLIT = 4
PARTS = 2


def pieces_of(C, W):
    even = W // SPLIT
    pieces = [(j, h * even, even) for j in range(C) for h in range(SPLIT)]
    if even > 128:
        pieces = [(0, 0, 128), (0, 128, even - 128)] + pieces[1:]
        j, offset, _ = pieces.pop()
        pieces += [(j, offset, even - 128), (j, offset + even - 128, 128)]
    return pieces


def kernel(R, S, anchor_h, rows_h, vel_h, feat_h, cot_h, w_h, m_h, s_h,
           na_o, mg_o, nv_o, nw_o, nm_o, ns_o,
           anchor, rows, vel, feat, cot, w, m, s, sib_rows, msg,
           in_sem, sib_send, sib_recv, y_send, cross_send, fwd_send, msg_recv,
           cot_own_send, cot_z_send, cot_x_send, cot_recv):
    C = R // 2
    me, at = lax.axis_index("replica"), lax.axis_index("shard")
    y, c = me // 2, me % 2
    sib = me + 1 - 2 * c
    partner = at + 1 - 2 * (at % 2)
    pos, length = at // 2, S // 2
    W = vel.shape[1]
    pieces = pieces_of(C, W)
    last = len(pieces) - 1
    depth = cot_h.shape[1]
    part_depth = depth // PARTS

    def columns(q, offset, width):
        return pl.ds(pl.multiple_of(q * W + offset, 128), width)

    def quarter(q):
        return pl.ds(pl.multiple_of(q * W, 128), W)

    def tokens(k):
        return pl.ds(pl.multiple_of(k * depth, depth), depth)

    def half_tokens(k, u):
        return pl.ds(pl.multiple_of(k * depth + u * part_depth, part_depth), part_depth)

    barrier = pltpu.get_barrier_semaphore()
    pl.semaphore_signal(barrier, inc=1, device_id={"replica": sib}, device_id_type=MESH)
    for t in range(1, C):
        pl.semaphore_signal(barrier, inc=1, device_id={"replica": lax.rem(me + 2 * t, R)}, device_id_type=MESH)
        pl.semaphore_signal(barrier, inc=1, device_id={"replica": lax.rem(sib + 2 * t, R)}, device_id_type=MESH)
    pl.semaphore_signal(barrier, inc=1, device_id={"shard": partner}, device_id_type=MESH)

    @pl.when(pos > 0)
    def _():
        pl.semaphore_signal(barrier, inc=1, device_id={"shard": at - 2}, device_id_type=MESH)

    @pl.when(pos < length - 1)
    def _():
        pl.semaphore_signal(barrier, inc=1, device_id={"shard": at + 2}, device_id_type=MESH)

    loads = {}
    slot = 0

    def load(name, src, dst):
        nonlocal slot
        copy = pltpu.make_async_copy(src, dst, in_sem.at[slot])
        copy.start()
        slot += 1
        loads[name] = copy

    load("cot", cot_h.at[0], cot.at[tokens(at)])
    for j in range(C):
        q = 2 * j + 1 - c
        load(("out", j), rows_h.at[0, :, quarter(q)], rows.at[:, quarter(q)])
    for j in range(C):
        q = 2 * j + c
        load(("keep", j), rows_h.at[0, :, quarter(q)], rows.at[:, quarter(q)])
    load("anchor", anchor_h, anchor)
    load("vel", vel_h, vel)
    load("feat", feat_h.at[0], feat)
    load("w", w_h.at[0], w)
    load("m", m_h.at[0], m)
    load("s", s_h.at[0], s)

    count = 2 + 2 * (C - 1) + (pos > 0).astype(jnp.int32) + (pos < length - 1).astype(jnp.int32)
    pl.semaphore_wait(barrier, count)

    def sib_copy(i):
        j, offset, width = pieces[i]
        return pltpu.make_async_remote_copy(
            src_ref=rows.at[:, columns(2 * j + 1 - c, offset, width)],
            dst_ref=sib_rows.at[j, :, pl.ds(offset, width)],
            send_sem=sib_send.at[i], recv_sem=sib_recv.at[i],
            device_id={"replica": sib}, device_id_type=MESH)

    def cot_copy(k, u, send_sem, target):
        return pltpu.make_async_remote_copy(
            src_ref=cot.at[half_tokens(k, u)], dst_ref=cot.at[half_tokens(k, u)],
            send_sem=send_sem.at[u], recv_sem=cot_recv.at[k, u],
            device_id={"shard": target}, device_id_type=MESH)

    for i, (j, offset, width) in enumerate(pieces):
        if offset == 0:
            loads[("out", j)].wait()
        sib_copy(i).start()

    loads["cot"].wait()
    cot_right = [cot_copy(at, u, cot_own_send.at[0], at + 2) for u in range(PARTS)]
    cot_left = [cot_copy(at, u, cot_own_send.at[1], at - 2) for u in range(PARTS)]
    cot_across = [cot_copy(at, u, cot_own_send.at[2], partner) for u in range(PARTS)]

    @pl.when(pos < length - 1)
    def _():
        for copy in cot_right:
            copy.start()

    @pl.when(pos > 0)
    def _():
        for copy in cot_left:
            copy.start()

    for copy in cot_across:
        copy.start()

    def slot_of(p, src, i):
        j, offset, width = pieces[i]
        return msg.at[p, src, j, :, pl.ds(offset, width)]

    def message(p, src, i, send_sem, target):
        return pltpu.make_async_remote_copy(
            src_ref=slot_of(p, src, i), dst_ref=slot_of(p, src, i),
            send_sem=send_sem, recv_sem=msg_recv.at[p, src, i],
            device_id={"replica": target}, device_id_type=MESH)

    def y_copy(t, i):
        return message(c, y, i, y_send.at[t - 1, i], lax.rem(me + 2 * t, R))

    def cross_copy(t):
        return message(c, y, last, cross_send.at[t - 1], lax.rem(sib + 2 * t, R))

    def to_sib(src, i):
        return message(c, src, i, fwd_send.at[src, i], sib)

    def arrival(p, src, i):
        return message(p, src, i, fwd_send.at[src, i], sib)

    c1 = outer_rate * (1.0 + momentum_keep)
    c2 = outer_rate * momentum_keep * momentum_keep
    share = c1 / R
    for i, (j, offset, width) in enumerate(pieces):
        if offset == 0:
            loads[("keep", j)].wait()
        if i == 0:
            loads["anchor"].wait()
            loads["vel"].wait()
        mine = y == j
        of_anchor = jnp.where(mine, 0.0, 2.0)
        of_rows = jnp.where(mine, share, -1.0)
        of_vel = jnp.where(mine, -c2, 0.0)
        sib_copy(i).wait_recv()
        cols = columns(2 * j + c, offset, width)
        part = slice(offset, offset + width)
        both = rows[:, cols].astype(jnp.float32) + sib_rows[j, :, part].astype(jnp.float32)
        value = of_anchor * anchor[:, cols] + of_rows * both
        value = value + of_vel * vel[:, part]
        msg[c, y, j, :, part] = value.astype(jnp.bfloat16)
        for t in range(1, C):
            y_copy(t, i).start()
            if i == last:
                cross_copy(t).start()
        to_sib(y, i).start()

    def finish(p, i):
        j, offset, width = pieces[i]
        cols = columns(2 * j + p, offset, width)
        part = slice(offset, offset + width)
        others = msg[p, (j + 1) % C, j, :, part].astype(jnp.float32)
        for t in range(2, C):
            others = others + msg[p, (j + t) % C, j, :, part].astype(jnp.float32)
        own = msg[p, j, j, :, part].astype(jnp.float32)
        new_anchor = (1.0 - 2.0 * share) * anchor[:, cols] + own - share * others
        na_o[:, cols] = new_anchor
        mg_o[0, :, cols] = (
            blend_keep * rows[:, cols].astype(jnp.float32) + (1.0 - blend_keep) * new_anchor
        ).astype(jnp.bfloat16)

    def finish_velocity(i):
        j, offset, width = pieces[i]

        @pl.when(y == j)
        def _():
            cols = columns(2 * j + c, offset, width)
            part = slice(offset, offset + width)
            total = 2.0 * anchor[:, cols] - (
                rows[:, cols].astype(jnp.float32) + sib_rows[j, :, part].astype(jnp.float32))
            for t in range(1, C):
                total = total + msg[c, (j + t) % C, j, :, part].astype(jnp.float32)
            nv_o[:, part] = momentum_keep * vel[:, part] + total / R

    def finish_sib(i):
        for src in range(C):
            arrival(1 - c, src, i).wait_recv()
        finish(1 - c, i)

    def cot_step(t, u):
        @pl.when(pos >= t)
        def _():
            k = at - 2 * t
            cot_copy(k, u, cot_x_send.at[0], partner).wait_recv()

            @pl.when(pos < length - 1)
            def _():
                cot_copy(k, u, cot_z_send.at[0, t - 1], at + 2).start()

            cot_copy(k, u, cot_x_send.at[k // 2], partner).start()

        @pl.when(pos + t < length)
        def _():
            k = at + 2 * t
            cot_copy(k, u, cot_x_send.at[0], partner).wait_recv()

            @pl.when(pos > 0)
            def _():
                cot_copy(k, u, cot_z_send.at[1, t - 1], at - 2).start()

            cot_copy(k, u, cot_x_send.at[k // 2], partner).start()

    def inner_step():
        for k in range(length):
            for u in range(PARTS):
                cot_copy(2 * k + 1 - at % 2, u, cot_x_send.at[0], partner).wait_recv()
        for name in ("feat", "w", "m", "s"):
            loads[name].wait()
        tile = min(256, w.shape[1])
        for n in range(w.shape[1] // tile):
            part = slice(n * tile, (n + 1) * tile)
            gradient = jnp.dot(feat[...], cot[:, part], preferred_element_type=jnp.float32)
            new_first = decay_first * m[:, part] + (1.0 - decay_first) * gradient
            new_second = decay_second * s[:, part] + (1.0 - decay_second) * gradient * gradient
            stepped = new_first / first_fix / (jnp.sqrt(new_second / second_fix) + epsilon)
            weight = w[:, part]
            nw_o[0, :, part] = weight - inner_rate * (stepped + weight_decay * weight)
            nm_o[0, :, part] = new_first
            ns_o[0, :, part] = new_second

    todo = [(t, u) for t in range(1, length) for u in range(PARTS)]
    for i in range(len(pieces)):
        while i < last and todo and 3 * (todo[0][0] - 1) + todo[0][1] <= i + 1:
            cot_step(*todo.pop(0))
        if i == last:
            for step in todo:
                cot_step(*step)
            inner_step()
            finish_sib(last - 1)
        for t in range(1, C):
            src = lax.rem(y + t, C)
            arrival(c, src, i).wait_recv()
            if i < last:
                to_sib(src, i).start()
        finish(c, i)
        finish_velocity(i)
        if 0 < i < last:
            finish_sib(i - 1)
    finish_sib(last)

    for i in range(len(pieces)):
        sib_copy(i).wait_send()
        for t in range(1, C):
            y_copy(t, i).wait_send()
            if i == last:
                cross_copy(t).wait_send()
            else:
                to_sib(lax.rem(y + t, C), i).wait_send()
        to_sib(y, i).wait_send()
    for copy in cot_across:
        copy.wait_send()

    @pl.when(pos < length - 1)
    def _():
        for copy in cot_right:
            copy.wait_send()

    @pl.when(pos > 0)
    def _():
        for copy in cot_left:
            copy.wait_send()

    for t, u in [(t, u) for t in range(1, length) for u in range(PARTS)]:
        @pl.when(pos >= t)
        def _():
            k = at - 2 * t

            @pl.when(pos < length - 1)
            def _():
                cot_copy(k, u, cot_z_send.at[0, t - 1], at + 2).wait_send()

            cot_copy(k, u, cot_x_send.at[k // 2], partner).wait_send()

        @pl.when(pos + t < length)
        def _():
            k = at + 2 * t

            @pl.when(pos > 0)
            def _():
                cot_copy(k, u, cot_z_send.at[1, t - 1], at - 2).wait_send()

            cot_copy(k, u, cot_x_send.at[k // 2], partner).wait_send()


def store_kernel(*refs):
    sems = refs[-1]
    count = (len(refs) - 1) // 2
    copies = []
    for source, target in zip(refs[:count], refs[count:-1]):
        rows = source.shape[-2]
        cuts = 3 if rows % 48 == 0 else 1
        for n in range(cuts):
            part = pl.ds(n * (rows // cuts), rows // cuts)
            index = (0, part) if len(source.shape) == 3 else (part,)
            copies.append(pltpu.make_async_copy(
                source.at[index], target.at[index], sems.at[len(copies)]))
    for copy in copies:
        copy.start()
    for copy in copies:
        copy.wait()


def store(*arrays):
    return pl.pallas_call(
        store_kernel,
        out_shape=tuple(jax.ShapeDtypeStruct(a.shape, a.dtype) for a in arrays),
        in_specs=[pl.BlockSpec(memory_space=pltpu.VMEM)] * len(arrays),
        out_specs=tuple(pl.BlockSpec(memory_space=pltpu.HBM) for _ in arrays),
        scratch_shapes=[pltpu.SemaphoreType.DMA((3 * len(arrays),))],
        compiler_params=pltpu.CompilerParams(vmem_limit_bytes=2**20),
    )(*arrays)


def local(R, S, anchor, replica_rows, outer_velocity, features, cotangent,
          inner_weight, first_moment, second_moment):
    C = R // 2
    depth_rows = anchor.shape[0]
    W = outer_velocity.shape[1]
    N = len(pieces_of(C, W))
    f32, bf16 = jnp.float32, jnp.bfloat16
    args = (anchor, replica_rows, outer_velocity, features, cotangent,
            inner_weight, first_moment, second_moment)
    outs = (anchor, replica_rows, outer_velocity, inner_weight, first_moment, second_moment)
    dma = pltpu.SemaphoreType.DMA
    length = S // 2
    room = 67043328 - sum(a.size * a.dtype.itemsize for a in outs) - 2**16
    results = pl.pallas_call(
        functools.partial(kernel, R, S),
        out_shape=tuple(pltpu.VMEM(a.shape, a.dtype) for a in outs),
        in_specs=[pl.BlockSpec(memory_space=pltpu.HBM)] * len(args),
        out_specs=tuple(pl.BlockSpec(memory_space=pltpu.VMEM) for _ in outs),
        scratch_shapes=[
            pltpu.VMEM(anchor.shape, f32),
            pltpu.VMEM(replica_rows.shape[1:], bf16),
            pltpu.VMEM(outer_velocity.shape, f32),
            pltpu.VMEM(features.shape[1:], bf16),
            pltpu.VMEM((S * cotangent.shape[1], cotangent.shape[2]), bf16),
            pltpu.VMEM(inner_weight.shape[1:], f32),
            pltpu.VMEM(inner_weight.shape[1:], f32),
            pltpu.VMEM(inner_weight.shape[1:], f32),
            pltpu.VMEM((C, depth_rows, W), bf16),
            pltpu.VMEM((2, C, C, depth_rows, W), bf16),
            dma((7 + 2 * C,)),
            dma((N,)),
            dma((N,)),
            dma((C - 1, N)),
            dma((C - 1,)),
            dma((C, N)),
            dma((2, C, N)),
            dma((3, PARTS)),
            dma((2, max(length - 1, 1), PARTS)),
            dma((length, PARTS)),
            dma((S, PARTS)),
        ],
        compiler_params=pltpu.CompilerParams(
            collective_id=0, has_side_effects=True, vmem_limit_bytes=room),
    )(*args)
    return store(*results)


def solution(mesh):
    in_specs = (
        P("shard", None),
        P("replica", "shard", None),
        P("shard", "replica"),
        P("replica", "shard", None),
        P("replica", "shard", None),
        P("replica", "shard", None),
        P("replica", "shard", None),
        P("replica", "shard", None),
    )
    out_specs = (
        P("shard", None),
        P("replica", "shard", None),
        P("shard", "replica"),
        P("replica", "shard", None),
        P("replica", "shard", None),
        P("replica", "shard", None),
    )
    body = functools.partial(local, mesh.shape["replica"], mesh.shape["shard"])
    return jax.shard_map(body, mesh=mesh, in_specs=in_specs, out_specs=out_specs, check_vma=False)
```

```python
import functools

import jax
import jax.numpy as jnp
from jax import lax
from jax.experimental import pallas as pl
from jax.experimental.pallas import tpu as pltpu
from jax.sharding import PartitionSpec as P

momentum_keep = 0.9
outer_rate = 0.7
blend_keep = 0.5
inner_rate = 0.01
decay_first = 0.9
decay_second = 0.95
weight_decay = 0.1
epsilon = 1e-08
first_fix = 1.0 - 0.9**10
second_fix = 1.0 - 0.95**10

MESH = pl.DeviceIdType.MESH
SPLIT = 4
PARTS = 4


def kernel(R, S, anchor_h, rows_h, vel_h, feat_h, cot_h, w_h, m_h, s_h,
           na_o, mg_o, nv_o, nw_o, nm_o, ns_o,
           anchor, rows, vel, feat, cot, w, m, s, sib_rows, msg,
           in_sem, sib_send, sib_recv, y_send, fwd_send, msg_recv,
           cot_own_send, cot_z_send, cot_x_send, cot_recv):
    C = R // 2
    H = SPLIT
    me, at = lax.axis_index("replica"), lax.axis_index("shard")
    y, c = me // 2, me % 2
    sib = me + 1 - 2 * c
    partner = at + 1 - 2 * (at % 2)
    pos, length = at // 2, S // 2
    W = vel.shape[1]
    piece = W // H
    depth = cot_h.shape[1]
    part_width = cot_h.shape[2] // PARTS

    def columns(q, h):
        return pl.ds(pl.multiple_of(q * W + h * piece, 128), piece)

    def quarter(q):
        return pl.ds(pl.multiple_of(q * W, 128), W)

    def tokens(k):
        return pl.ds(pl.multiple_of(k * depth, depth), depth)

    def block_part(k, u):
        return cot.at[tokens(k), pl.ds(u * part_width, part_width)]

    barrier = pltpu.get_barrier_semaphore()
    pl.semaphore_signal(barrier, inc=1, device_id={"replica": sib}, device_id_type=MESH)
    for t in range(1, C):
        pl.semaphore_signal(barrier, inc=1, device_id={"replica": lax.rem(me + 2 * t, R)}, device_id_type=MESH)
    pl.semaphore_signal(barrier, inc=1, device_id={"shard": partner}, device_id_type=MESH)

    @pl.when(pos > 0)
    def _():
        pl.semaphore_signal(barrier, inc=1, device_id={"shard": at - 2}, device_id_type=MESH)

    @pl.when(pos < length - 1)
    def _():
        pl.semaphore_signal(barrier, inc=1, device_id={"shard": at + 2}, device_id_type=MESH)

    loads = {}
    slot = 0

    def load(name, src, dst):
        nonlocal slot
        copy = pltpu.make_async_copy(src, dst, in_sem.at[slot])
        copy.start()
        slot += 1
        loads[name] = copy

    load("cot", cot_h.at[0], cot.at[tokens(at)])
    for j in range(C):
        q = 2 * j + 1 - c
        load(("out", j), rows_h.at[0, :, quarter(q)], rows.at[:, quarter(q)])
    for j in range(C):
        q = 2 * j + c
        load(("keep", j), rows_h.at[0, :, quarter(q)], rows.at[:, quarter(q)])
    load("anchor", anchor_h, anchor)
    load("vel", vel_h, vel)
    load("feat", feat_h.at[0], feat)
    load("w", w_h.at[0], w)
    load("m", m_h.at[0], m)
    load("s", s_h.at[0], s)

    count = 2 + (C - 1) + (pos > 0).astype(jnp.int32) + (pos < length - 1).astype(jnp.int32)
    pl.semaphore_wait(barrier, count)

    def sib_copy(j, h):
        return pltpu.make_async_remote_copy(
            src_ref=rows.at[:, columns(2 * j + 1 - c, h)], dst_ref=sib_rows.at[j, h],
            send_sem=sib_send.at[j, h], recv_sem=sib_recv.at[j, h],
            device_id={"replica": sib}, device_id_type=MESH)

    def cot_copy(k, u, send_sem, target):
        return pltpu.make_async_remote_copy(
            src_ref=block_part(k, u), dst_ref=block_part(k, u),
            send_sem=send_sem.at[u], recv_sem=cot_recv.at[k, u],
            device_id={"shard": target}, device_id_type=MESH)

    for j in range(C):
        loads[("out", j)].wait()
        for h in range(H):
            sib_copy(j, h).start()

    loads["cot"].wait()
    cot_right = [cot_copy(at, u, cot_own_send.at[0], at + 2) for u in range(PARTS)]
    cot_left = [cot_copy(at, u, cot_own_send.at[1], at - 2) for u in range(PARTS)]
    cot_across = [cot_copy(at, u, cot_own_send.at[2], partner) for u in range(PARTS)]

    @pl.when(pos < length - 1)
    def _():
        for copy in cot_right:
            copy.start()

    @pl.when(pos > 0)
    def _():
        for copy in cot_left:
            copy.start()

    for copy in cot_across:
        copy.start()

    def y_copy(t, j, h):
        return pltpu.make_async_remote_copy(
            src_ref=msg.at[c, y, j, h], dst_ref=msg.at[c, y, j, h],
            send_sem=y_send.at[t - 1, j, h], recv_sem=msg_recv.at[c, y, j, h],
            device_id={"replica": lax.rem(me + 2 * t, R)}, device_id_type=MESH)

    def to_sib(src, j, h):
        return pltpu.make_async_remote_copy(
            src_ref=msg.at[c, src, j, h], dst_ref=msg.at[c, src, j, h],
            send_sem=fwd_send.at[src, j, h], recv_sem=msg_recv.at[c, src, j, h],
            device_id={"replica": sib}, device_id_type=MESH)

    def arrival(p, src, j, h):
        return pltpu.make_async_remote_copy(
            src_ref=msg.at[p, src, j, h], dst_ref=msg.at[p, src, j, h],
            send_sem=fwd_send.at[src, j, h], recv_sem=msg_recv.at[p, src, j, h],
            device_id={"replica": sib}, device_id_type=MESH)

    c1 = outer_rate * (1.0 + momentum_keep)
    c2 = outer_rate * momentum_keep * momentum_keep
    share = c1 / R
    for j in range(C):
        loads[("keep", j)].wait()
        if j == 0:
            loads["anchor"].wait()
            loads["vel"].wait()
        mine = y == j
        of_anchor = jnp.where(mine, 0.0, 2.0)
        of_rows = jnp.where(mine, share, -1.0)
        of_vel = jnp.where(mine, -c2, 0.0)
        for h in range(H):
            sib_copy(j, h).wait_recv()
            cols = columns(2 * j + c, h)
            both = rows[:, cols].astype(jnp.float32) + sib_rows[j, h].astype(jnp.float32)
            value = of_anchor * anchor[:, cols] + of_rows * both
            value = value + of_vel * vel[:, h * piece:(h + 1) * piece]
            msg[c, y, j, h] = value.astype(jnp.bfloat16)
            for t in range(1, C):
                y_copy(t, j, h).start()
            to_sib(y, j, h).start()

    def finish(p, j, h):
        cols = columns(2 * j + p, h)
        others = msg[p, (j + 1) % C, j, h].astype(jnp.float32)
        for t in range(2, C):
            others = others + msg[p, (j + t) % C, j, h].astype(jnp.float32)
        own = msg[p, j, j, h].astype(jnp.float32)
        new_anchor = (1.0 - 2.0 * share) * anchor[:, cols] + own - share * others
        na_o[:, cols] = new_anchor
        mg_o[0, :, cols] = (
            blend_keep * rows[:, cols].astype(jnp.float32) + (1.0 - blend_keep) * new_anchor
        ).astype(jnp.bfloat16)

    def finish_velocity(j, h):
        @pl.when(y == j)
        def _():
            cols = columns(2 * j + c, h)
            part = slice(h * piece, (h + 1) * piece)
            total = 2.0 * anchor[:, cols] - (
                rows[:, cols].astype(jnp.float32) + sib_rows[j, h].astype(jnp.float32))
            for t in range(1, C):
                total = total + msg[c, (j + t) % C, j, h].astype(jnp.float32)
            nv_o[:, part] = momentum_keep * vel[:, part] + total / R

    def finish_sib(j, h):
        for src in range(C):
            arrival(1 - c, src, j, h).wait_recv()
        finish(1 - c, j, h)

    def cot_step(t, u):
        @pl.when(pos >= t)
        def _():
            k = at - 2 * t
            cot_copy(k, u, cot_x_send.at[0], partner).wait_recv()

            @pl.when(pos < length - 1)
            def _():
                cot_copy(k, u, cot_z_send.at[0, t - 1], at + 2).start()

            cot_copy(k, u, cot_x_send.at[k // 2], partner).start()

        @pl.when(pos + t < length)
        def _():
            k = at + 2 * t
            cot_copy(k, u, cot_x_send.at[0], partner).wait_recv()

            @pl.when(pos > 0)
            def _():
                cot_copy(k, u, cot_z_send.at[1, t - 1], at - 2).start()

            cot_copy(k, u, cot_x_send.at[k // 2], partner).start()

    pieces = [(j, h) for j in range(C) for h in range(H)]
    todo = [(t, u) for t in range(1, length) for u in range(PARTS)]
    before = None
    for i, (j, h) in enumerate(pieces):
        while todo and 3 * (todo[0][0] - 1) + todo[0][1] // 2 <= i + 2:
            cot_step(*todo.pop(0))
        for t in range(1, C):
            src = lax.rem(y + t, C)
            arrival(c, src, j, h).wait_recv()
            to_sib(src, j, h).start()
        finish(c, j, h)
        finish_velocity(j, h)
        if before is not None:
            finish_sib(*before)
        before = (j, h)
    for step in todo:
        cot_step(*step)

    for k in range(length):
        for u in range(PARTS):
            cot_copy(2 * k + 1 - at % 2, u, cot_x_send.at[0], partner).wait_recv()
    for name in ("feat", "w", "m", "s"):
        loads[name].wait()
    tile = min(256, w.shape[1])
    for n in range(w.shape[1] // tile):
        part = slice(n * tile, (n + 1) * tile)
        gradient = jnp.dot(feat[...], cot[:, part], preferred_element_type=jnp.float32)
        new_first = decay_first * m[:, part] + (1.0 - decay_first) * gradient
        new_second = decay_second * s[:, part] + (1.0 - decay_second) * gradient * gradient
        stepped = new_first / first_fix / (jnp.sqrt(new_second / second_fix) + epsilon)
        weight = w[:, part]
        nw_o[0, :, part] = weight - inner_rate * (stepped + weight_decay * weight)
        nm_o[0, :, part] = new_first
        ns_o[0, :, part] = new_second

    finish_sib(*before)

    for j, h in pieces:
        sib_copy(j, h).wait_send()
        for t in range(1, C):
            y_copy(t, j, h).wait_send()
        for src in range(C):
            to_sib(src, j, h).wait_send()
    for copy in cot_across:
        copy.wait_send()

    @pl.when(pos < length - 1)
    def _():
        for copy in cot_right:
            copy.wait_send()

    @pl.when(pos > 0)
    def _():
        for copy in cot_left:
            copy.wait_send()

    for t, u in [(t, u) for t in range(1, length) for u in range(PARTS)]:
        @pl.when(pos >= t)
        def _():
            k = at - 2 * t

            @pl.when(pos < length - 1)
            def _():
                cot_copy(k, u, cot_z_send.at[0, t - 1], at + 2).wait_send()

            cot_copy(k, u, cot_x_send.at[k // 2], partner).wait_send()

        @pl.when(pos + t < length)
        def _():
            k = at + 2 * t

            @pl.when(pos > 0)
            def _():
                cot_copy(k, u, cot_z_send.at[1, t - 1], at - 2).wait_send()

            cot_copy(k, u, cot_x_send.at[k // 2], partner).wait_send()


def store_kernel(*refs):
    sems = refs[-1]
    count = (len(refs) - 1) // 2
    copies = []
    for source, target in zip(refs[:count], refs[count:-1]):
        rows = source.shape[-2]
        cuts = 3 if rows % 48 == 0 else 1
        for n in range(cuts):
            part = pl.ds(n * (rows // cuts), rows // cuts)
            index = (0, part) if len(source.shape) == 3 else (part,)
            copies.append(pltpu.make_async_copy(
                source.at[index], target.at[index], sems.at[len(copies)]))
    for copy in copies:
        copy.start()
    for copy in copies:
        copy.wait()


def store(*arrays):
    return pl.pallas_call(
        store_kernel,
        out_shape=tuple(jax.ShapeDtypeStruct(a.shape, a.dtype) for a in arrays),
        in_specs=[pl.BlockSpec(memory_space=pltpu.VMEM)] * len(arrays),
        out_specs=tuple(pl.BlockSpec(memory_space=pltpu.HBM) for _ in arrays),
        scratch_shapes=[pltpu.SemaphoreType.DMA((3 * len(arrays),))],
        compiler_params=pltpu.CompilerParams(vmem_limit_bytes=2**20),
    )(*arrays)


def local(R, S, anchor, replica_rows, outer_velocity, features, cotangent,
          inner_weight, first_moment, second_moment):
    C, H = R // 2, SPLIT
    depth_rows = anchor.shape[0]
    W = outer_velocity.shape[1]
    f32, bf16 = jnp.float32, jnp.bfloat16
    args = (anchor, replica_rows, outer_velocity, features, cotangent,
            inner_weight, first_moment, second_moment)
    outs = (anchor, replica_rows, outer_velocity, inner_weight, first_moment, second_moment)
    dma = pltpu.SemaphoreType.DMA
    length = S // 2
    room = 67043328 - sum(a.size * a.dtype.itemsize for a in outs) - 2**16
    results = pl.pallas_call(
        functools.partial(kernel, R, S),
        out_shape=tuple(pltpu.VMEM(a.shape, a.dtype) for a in outs),
        in_specs=[pl.BlockSpec(memory_space=pltpu.HBM)] * len(args),
        out_specs=tuple(pl.BlockSpec(memory_space=pltpu.VMEM) for _ in outs),
        scratch_shapes=[
            pltpu.VMEM(anchor.shape, f32),
            pltpu.VMEM(replica_rows.shape[1:], bf16),
            pltpu.VMEM(outer_velocity.shape, f32),
            pltpu.VMEM(features.shape[1:], bf16),
            pltpu.VMEM((S * cotangent.shape[1], cotangent.shape[2]), bf16),
            pltpu.VMEM(inner_weight.shape[1:], f32),
            pltpu.VMEM(inner_weight.shape[1:], f32),
            pltpu.VMEM(inner_weight.shape[1:], f32),
            pltpu.VMEM((C, H, depth_rows, W // H), bf16),
            pltpu.VMEM((2, C, C, H, depth_rows, W // H), bf16),
            dma((7 + 2 * C,)),
            dma((C, H)),
            dma((C, H)),
            dma((C - 1, C, H)),
            dma((C, C, H)),
            dma((2, C, C, H)),
            dma((3, PARTS)),
            dma((2, max(length - 1, 1), PARTS)),
            dma((length, PARTS)),
            dma((S, PARTS)),
        ],
        compiler_params=pltpu.CompilerParams(
            collective_id=0, has_side_effects=True, vmem_limit_bytes=room),
    )(*args)
    return store(*results)


def solution(mesh):
    in_specs = (
        P("shard", None),
        P("replica", "shard", None),
        P("shard", "replica"),
        P("replica", "shard", None),
        P("replica", "shard", None),
        P("replica", "shard", None),
        P("replica", "shard", None),
        P("replica", "shard", None),
    )
    out_specs = (
        P("shard", None),
        P("replica", "shard", None),
        P("shard", "replica"),
        P("replica", "shard", None),
        P("replica", "shard", None),
        P("replica", "shard", None),
    )
    body = functools.partial(local, mesh.shape["replica"], mesh.shape["shard"])
    return jax.shard_map(body, mesh=mesh, in_specs=in_specs, out_specs=out_specs, check_vma=False)
```
